32 devices in a mesh: rep: 1 (over z), col: 4 (over y), row: 8 (over x, core).
Axes of the slice: x: 4, y: 4, z: 1, core: 2. Of those that a mesh axis runs over, the one named last changes fastest.
The devices are a block of a 4x4x8 slice.
Arguments:
- hidden_0: bfloat16 [128, 2048], P('rep', 'row')
- hidden_1: bfloat16 [128, 2048], P('rep', 'row')
- positions: int32 [128], P(('rep', 'row'))
- lengths: int32 [128], P(('rep', 'row'))
- cache_k: bfloat16 [2, 128, 1024, 8, 64], P(None, ('rep', 'row'), None, 'col')
- cache_v: bfloat16 [2, 128, 1024, 8, 64], P(None, ('rep', 'row'), None, 'col')
- norm_attn: bfloat16 [2, 2048], P(None, 'row')
- norm_mlp: bfloat16 [2, 2048], P(None, 'row')
- w_query: bfloat16 [2, 2048, 2048], P(None, 'row', 'col')
- w_key: bfloat16 [2, 2048, 512], P(None, 'row', 'col')
- w_value: bfloat16 [2, 2048, 512], P(None, 'row', 'col')
- w_out: bfloat16 [2, 2048, 2048], P(None, 'row', 'col')
- w_gate: bfloat16 [2, 2048, 8192], P(None, 'row', 'col')
- w_up: bfloat16 [2, 2048, 8192], P(None, 'row', 'col')
- w_down: bfloat16 [2, 8192, 2048], P(None, 'row', 'col')
Outputs:
- output 1: bfloat16 [128, 2048], P('rep', 'row')
- output 2: bfloat16 [128, 2048], P('rep', 'row')
- output 3: bfloat16 [2, 128, 1024, 8, 64], P(None, ('rep', 'row'), None, 'col')
- output 4: bfloat16 [2, 128, 1024, 8, 64], P(None, ('rep', 'row'), None, 'col')
All inputs are finite; a program needn't handle non-finite values.
Results may differ from the reference program's by a relative error of at most 0.02.
Values are sent between devices in bfloat16 or wider.
A program may use at most 768 MiB of HBM per device.

```python
import math
import jax
import jax.numpy as jnp
from jax import lax

BATCH = 128
CTX_LEN = 1024
D_MODEL = 2048
HEADS = 32
KV_HEADS = 8
HEAD_DIM = 64
FF_DIM = 8192
LAYERS = 2
ROPE_BASE = 1000000
EPS = 1e-05
GROUP_SIZE = HEADS // KV_HEADS
Q_WIDTH = HEADS * HEAD_DIM
KV_WIDTH = KV_HEADS * HEAD_DIM
LEN_BITS = int(math.log2(CTX_LEN))


def draw_lengths(key):
    key_exp, key_len, key_pick, key_pos = jax.random.split(key, 4)
    exponent = jax.random.randint(key_exp, (BATCH,), 0, LEN_BITS + 1)
    length_cap = jnp.minimum(jnp.left_shift(jnp.ones((BATCH,), jnp.int32), exponent), CTX_LEN - 2)
    lengths = 1 + jax.random.randint(key_len, (BATCH,), 0, length_cap)
    shuffled = jax.random.permutation(key_pick, BATCH)
    lengths = lengths.at[shuffled[0]].set(CTX_LEN - 2).at[shuffled[1]].set(1)
    positions = lengths + jax.random.randint(key_pos, (BATCH,), 0, CTX_LEN)
    return positions.astype(jnp.int32), lengths.astype(jnp.int32)


def normal_weight(key, shape, fan_in):
    return (jax.random.normal(key, shape, jnp.float32) * fan_in ** -0.5).astype(jnp.bfloat16)


def setup_inputs(seed: int = 0, part: int = 0) -> dict:
    part_keys = jax.random.split(jax.random.fold_in(jax.random.key(seed), part), 5)
    weight_keys = jax.random.split(jax.random.key(seed + 1), 9)
    positions, lengths = draw_lengths(part_keys[0])
    cache_shape = (LAYERS, BATCH, CTX_LEN, KV_HEADS, HEAD_DIM)
    return {
        'hidden_0': jax.random.normal(part_keys[1], (BATCH, D_MODEL), jnp.float32).astype(jnp.bfloat16),
        'hidden_1': jax.random.normal(part_keys[2], (BATCH, D_MODEL), jnp.float32).astype(jnp.bfloat16),
        'positions': positions,
        'lengths': lengths,
        'cache_k': jax.random.normal(part_keys[3], cache_shape, jnp.float32).astype(jnp.bfloat16),
        'cache_v': jax.random.normal(part_keys[4], cache_shape, jnp.float32).astype(jnp.bfloat16),
        'norm_attn': (1.0 + 0.4 * jax.random.normal(weight_keys[0], (LAYERS, D_MODEL), jnp.float32)).astype(jnp.bfloat16),
        'norm_mlp': (1.0 + 0.4 * jax.random.normal(weight_keys[1], (LAYERS, D_MODEL), jnp.float32)).astype(jnp.bfloat16),
        'w_query': normal_weight(weight_keys[2], (LAYERS, D_MODEL, Q_WIDTH), D_MODEL),
        'w_key': normal_weight(weight_keys[3], (LAYERS, D_MODEL, KV_WIDTH), D_MODEL),
        'w_value': normal_weight(weight_keys[4], (LAYERS, D_MODEL, KV_WIDTH), D_MODEL),
        'w_out': normal_weight(weight_keys[5], (LAYERS, Q_WIDTH, D_MODEL), Q_WIDTH),
        'w_gate': normal_weight(weight_keys[6], (LAYERS, D_MODEL, FF_DIM), D_MODEL),
        'w_up': normal_weight(weight_keys[7], (LAYERS, D_MODEL, FF_DIM), D_MODEL),
        'w_down': normal_weight(weight_keys[8], (LAYERS, FF_DIM, D_MODEL), FF_DIM),
    }


def rms_norm(hidden, gain):
    hidden_f = hidden.astype(jnp.float32)
    scale = lax.rsqrt(jnp.mean(hidden_f * hidden_f, axis=-1, keepdims=True) + EPS)
    return (hidden_f * scale * gain.astype(jnp.float32)).astype(jnp.bfloat16)


def matmul_bf16(left, right):
    return jnp.dot(left, right, preferred_element_type=jnp.float32).astype(jnp.bfloat16)


def rope_rotate(vectors, positions):
    half = HEAD_DIM // 2
    inv_freq = jnp.power(jnp.float32(ROPE_BASE), -jnp.arange(half, dtype=jnp.float32) * 2.0 / HEAD_DIM)
    angles = positions.astype(jnp.float32)[:, None, None] * inv_freq
    cosine = jnp.cos(angles)
    sine = jnp.sin(angles)
    first = vectors[..., :half]
    second = vectors[..., half:]
    return jnp.concatenate([first * cosine - second * sine, second * cosine + first * sine], axis=-1).astype(jnp.bfloat16)


def attend_row(row_inputs):
    query, keys, vals, last_slot = row_inputs
    scores = jnp.einsum('kgd,lkd->kgl', query.astype(jnp.float32), keys.astype(jnp.float32)) * (HEAD_DIM ** -0.5)
    valid = jnp.arange(CTX_LEN)[None, None, :] <= last_slot
    probs = jax.nn.softmax(jnp.where(valid, scores, -jnp.inf), axis=-1).astype(jnp.bfloat16)
    return jnp.einsum('kgl,lkd->kgd', probs.astype(jnp.float32), vals.astype(jnp.float32)).astype(jnp.bfloat16)


def decoder_layer(hidden, layer_weights, keys_layer, vals_layer, positions, slots):
    norm_attn, norm_mlp, w_query, w_key, w_value, w_out, w_gate, w_up, w_down = layer_weights
    batch = hidden.shape[0]
    normed = rms_norm(hidden, norm_attn)
    query = rope_rotate(matmul_bf16(normed, w_query).astype(jnp.float32).reshape(batch, HEADS, HEAD_DIM), positions)
    key_new = rope_rotate(matmul_bf16(normed, w_key).astype(jnp.float32).reshape(batch, KV_HEADS, HEAD_DIM), positions)
    value_new = matmul_bf16(normed, w_value).reshape(batch, KV_HEADS, HEAD_DIM)
    rows = jnp.arange(batch)
    keys_layer = keys_layer.at[rows, slots].set(key_new)
    vals_layer = vals_layer.at[rows, slots].set(value_new)
    attended = lax.map(attend_row, (query.reshape(batch, KV_HEADS, GROUP_SIZE, HEAD_DIM), keys_layer, vals_layer, slots))
    attn_out = matmul_bf16(attended.reshape(batch, Q_WIDTH), w_out)
    hidden = (hidden.astype(jnp.float32) + attn_out.astype(jnp.float32)).astype(jnp.bfloat16)
    normed = rms_norm(hidden, norm_mlp)
    gate = matmul_bf16(normed, w_gate).astype(jnp.float32)
    up_proj = matmul_bf16(normed, w_up).astype(jnp.float32)
    activated = (jax.nn.silu(gate) * up_proj).astype(jnp.bfloat16)
    down_out = matmul_bf16(activated, w_down)
    hidden = (hidden.astype(jnp.float32) + down_out.astype(jnp.float32)).astype(jnp.bfloat16)
    return hidden, keys_layer, vals_layer


def run_step(hidden, positions, slots, cache_k, cache_v, weights):
    def layer_body(carry, layer_inputs):
        layer_weights, keys_layer, vals_layer = layer_inputs
        carry, keys_layer, vals_layer = decoder_layer(carry, layer_weights, keys_layer, vals_layer, positions, slots)
        return carry, (keys_layer, vals_layer)
    hidden, caches = lax.scan(layer_body, hidden, (weights, cache_k, cache_v))
    return hidden, caches[0], caches[1]


def reference(hidden_0, hidden_1, positions, lengths, cache_k, cache_v, norm_attn, norm_mlp, w_query, w_key, w_value, w_out, w_gate, w_up, w_down):
    weights = (norm_attn, norm_mlp, w_query, w_key, w_value, w_out, w_gate, w_up, w_down)
    output_0, cache_k, cache_v = run_step(hidden_0, positions, lengths, cache_k, cache_v, weights)
    output_1, cache_k, cache_v = run_step(hidden_1, positions + 1, lengths + 1, cache_k, cache_v, weights)
    return (output_0, output_1, cache_k, cache_v)
```

```python
import functools

import jax
import jax.numpy as jnp
import numpy as np
from jax import lax
from jax.experimental import pallas as pl
from jax.experimental.pallas import tpu as pltpu
from jax.sharding import PartitionSpec as P

ROPE_BASE = 1000000.0
EPS = 1e-05
MESH = pl.DeviceIdType.MESH
BF16 = jnp.bfloat16
F32 = jnp.float32
STEPS = 2


def at_multiple(index, size):
    return pl.ds(pl.multiple_of(index * size, size), size)


def decode_kernel(
        h0, h1, pos, lens, kc, vc, gain_a, gain_m, freq, wq, wk, wv, wo, wg, wu, wd,
        out0, out1, new_kv,
        hin, gsrc, gful, kbuf, vbuf, wqkv, wov, wgu, wdv,
        xst, xmid, nst1, nin1, qs, qr, ob, oin, os_, orr, nst2, nin2, gs, gr, aa, ab, ds_, dr,
        qf, of, kn, vn, cs, sn,
        hin_sem, kv_sem, w_sem, wx_send, wx_recv, init_send, init_recv, g_send, g_recv,
        n1_send, n1_recv, q_send, q_recv, o_send, o_recv, ro_send, ro_recv, x_send, x_recv,
        n2_send, n2_recv, gu_send, gu_recv, aa_send, aa_recv, ab_send, ab_recv, rd_send, rd_recv,
        x2_send, x2_recv, out_sem):
    layers = wq.shape[0]
    rows_n = lax.axis_size('row')
    cols_n = lax.axis_size('col')
    chips_n = rows_n // 2
    r = lax.axis_index('row')
    c = lax.axis_index('col')
    chip, core = r // 2, r % 2
    batch, ks = h0.shape
    hb = batch // rows_n
    width = ks * rows_n
    cw = wo.shape[-1]
    q_w = wq.shape[-1]
    kv_w = wk.shape[-1]
    qkv_w = q_w + 2 * kv_w
    ff = wg.shape[-1]
    fh = ff // 2
    cb = batch // chips_n
    ctx = kc.shape[-1]
    hins = (h0, h1)
    outs = (out0, out1)

    def peer_copy(src, dst, send_sem, recv_sem, row, col):
        return pltpu.make_async_remote_copy(
            src_ref=src, dst_ref=dst, send_sem=send_sem, recv_sem=recv_sem,
            device_id={'row': row, 'col': col}, device_id_type=MESH)

    def wait_recv(ref, sem):
        peer_copy(ref, ref, sem, sem, r, c).wait_recv()

    def wait_send(ref, sem):
        peer_copy(ref, ref, sem, sem, r, c).wait_send()

    for s in range(STEPS):
        pltpu.make_async_copy(hins[s], hin.at[s], hin_sem.at[s]).start()
    for l in range(layers):
        for src, lo, n in ((wq, 0, q_w), (wk, q_w, kv_w), (wv, q_w + kv_w, kv_w)):
            pltpu.make_async_copy(src.at[l], wqkv.at[l, :, pl.ds(lo, n)], w_sem.at[l, 0]).start()
        pltpu.make_async_copy(kc.at[l], kbuf.at[l], kv_sem.at[l, 0]).start()
        pltpu.make_async_copy(vc.at[l], vbuf.at[l], kv_sem.at[l, 1]).start()
        pltpu.make_async_copy(wo.at[l], wov.at[l], w_sem.at[l, 1]).start()
        for k, src in enumerate((wg, wu)):
            pltpu.make_async_copy(src.at[l, :, at_multiple(core, fh)],
                                  wgu.at[l, at_multiple(core, ks), pl.ds(k * fh, fh)], w_sem.at[l, 2]).start()
        pltpu.make_async_copy(wd.at[l], wdv.at[l], w_sem.at[l, 3]).start()
    gsrc[...] = jnp.concatenate([gain_a[...].astype(F32), gain_m[...].astype(F32),
                                 jnp.zeros((gsrc.shape[0] - 2 * layers, ks), F32)], axis=0)
    gful[:, at_multiple(r, ks)] = gsrc[...]

    barrier = pltpu.get_barrier_semaphore()
    for k in range(1, rows_n * cols_n):
        other = lax.rem(r * cols_n + c + k, rows_n * cols_n)
        pl.semaphore_signal(barrier, inc=1, device_id={'row': other // cols_n, 'col': lax.rem(other, cols_n)},
                            device_id_type=MESH)
    pl.semaphore_wait(barrier, rows_n * cols_n - 1)

    def row_peer(d):
        return lax.rem(r + d, rows_n)

    for d in range(1, rows_n):
        peer_copy(gsrc, gful.at[:, at_multiple(r, ks)], g_send, g_recv, row_peer(d), c).start()
    for s in range(STEPS):
        pltpu.make_async_copy(hins[s], hin.at[s], hin_sem.at[s]).wait()
        for d in range(1, rows_n):
            peer_copy(hin.at[s, at_multiple(row_peer(d), hb), :], xst.at[0, s, :, at_multiple(r, ks)],
                      init_send.at[s], init_recv.at[s], row_peer(d), c).start()
        xst[0, s, :, at_multiple(r, ks)] = hin[s, at_multiple(r, hb), :]
    for l in range(layers):
        for k, src in enumerate((wg, wu)):
            peer_copy(src.at[l, :, at_multiple(1 - core, fh)],
                      wgu.at[l, at_multiple(core, ks), pl.ds(k * fh, fh)],
                      wx_send.at[l], wx_recv.at[l], r + 1 - 2 * core, c).start()

    lane = lax.broadcasted_iota(jnp.int32, (hb, 128), 1)
    sub = lax.broadcasted_iota(jnp.int32, (hb, 128), 0)
    first_half = lax.rem(lane, 64) < 32
    pos_col = jnp.zeros((hb, 128), jnp.int32)
    for b in range(hb):
        pos_col = jnp.where(sub == b, pos[b], pos_col)
    for s in range(STEPS):
        angle = (pos_col + s).astype(F32) * freq[...]
        cs[s] = jnp.cos(angle)
        sine = jnp.sin(angle)
        sn[s] = jnp.where(first_half, -sine, sine)

    def norm_rows(x, gain_row):
        xf = x.astype(F32)
        scale = lax.rsqrt(jnp.sum(xf * xf, axis=-1, keepdims=True) * (1.0 / width) + EPS)
        return (xf * scale * gful[pl.ds(gain_row, 1), :]).astype(BF16)

    def send_n1(l, s):
        for d in range(1, rows_n):
            peer_copy(nst1.at[l, s, :, at_multiple(row_peer(d), ks)], nin1.at[l, s, at_multiple(r, hb), :],
                      n1_send.at[l, s], n1_recv.at[l, s], row_peer(d), c).start()
        nin1[l, s, at_multiple(r, hb), :] = nst1[l, s, :, at_multiple(r, ks)]

    wait_recv(gful.at[:, pl.ds(0, (rows_n - 1) * ks)], g_recv)
    for s in range(STEPS):
        wait_recv(xst.at[0, s, :, pl.ds(0, (rows_n - 1) * ks)], init_recv.at[s])
        nst1[0, s] = norm_rows(xst[0, s], 0)
        send_n1(0, s)

    def reduce_rows(stage, recv, sem, l, s):
        wait_recv(recv.at[l, s], sem.at[l, s])
        total = stage[l, s, at_multiple(r, hb), :].astype(F32)
        for d in range(rows_n - 1):
            total += recv[l, s, d].astype(F32)
        return total

    def scatter_rows(stage, recv, send_sem, recv_sem, l, s):
        for d in range(1, rows_n):
            peer_copy(stage.at[l, s, at_multiple(row_peer(d), hb), :], recv.at[l, s, d - 1],
                      send_sem.at[l, s], recv_sem.at[l, s], row_peer(d), c).start()

    def rope(x, s):
        turned = jnp.where(first_half, pltpu.roll(x, 96, 1), pltpu.roll(x, 32, 1))
        return (x * cs[s] + turned * sn[s]).astype(BF16).astype(F32)

    def attention(l, s):
        qkv = reduce_rows(qs, qr, q_recv, l, s).astype(BF16).astype(F32)
        key = rope(qkv[:, q_w:q_w + kv_w], s)
        val = qkv[:, q_w + kv_w:]
        kn[s] = key
        vn[s] = val
        new_kv[l, s, 0] = key
        new_kv[l, s, 1] = val
        for t in range(4):
            kv, pair = t // 2, t % 2
            y = rope(qkv[:, 128 * t:128 * t + 128], s)
            for e in range(2):
                z = y if e == kv else pltpu.roll(y, 64, 1)
                qf[pl.ds(kv * 4 + pair * 2 + e, hb, stride=8), :] = jnp.where(lane // 64 == kv, z, 0.0)
        slot = lax.broadcasted_iota(jnp.int32, (8, ctx), 1)

        def group(gi, carry):
            for u in range(4):
                b = gi * 4 + u
                qv = qf[at_multiple(b, 8), :]
                sc = jnp.dot(qv.astype(BF16), kbuf[l, b], preferred_element_type=F32) * 0.125
                sc = jnp.where(slot < lens[b], sc, -jnp.inf)
                top = jnp.max(sc, axis=-1, keepdims=True)
                news = []
                for e in range(s + 1):
                    news.append(jnp.sum(qv * kn[e, pl.ds(b, 1), :], axis=-1, keepdims=True) * 0.125)
                    top = jnp.maximum(top, news[e])
                p = jnp.exp(sc - top)
                news = [jnp.exp(x - top) for x in news]
                inv = 1.0 / functools.reduce(lambda x, y: x + y, news, jnp.sum(p, axis=-1, keepdims=True))
                o = lax.dot_general((p * inv).astype(BF16), vbuf[l, b], (((1,), (1,)), ((), ())),
                                    preferred_element_type=F32)
                for e in range(s + 1):
                    o += (news[e] * inv).astype(BF16).astype(F32) * vn[e, pl.ds(b, 1), :]
                of[at_multiple(b, 8), :] = o
            return carry

        lax.fori_loop(0, hb // 4, group, 0)
        for t in range(4):
            kv, pair = t // 2, t % 2
            lo = of[pl.ds(kv * 4 + pair * 2, hb, stride=8), :]
            hi = of[pl.ds(kv * 4 + pair * 2 + 1, hb, stride=8), :]
            lo = lo if kv == 0 else pltpu.roll(lo, 64, 1)
            hi = hi if kv == 1 else pltpu.roll(hi, 64, 1)
            ob[l, s, :, 128 * t:128 * t + 128] = jnp.where(lane < 64, lo, hi).astype(BF16)
        for j in range(2):
            for d in range(cols_n):
                copy = peer_copy(ob.at[l, s, :, pl.ds(j * ks, ks)], oin.at[l, s, at_multiple(r, hb), :],
                                 o_send.at[l, s], o_recv.at[l, s], 2 * c + j, lax.rem(c + d, cols_n))
                if d == 0:
                    mine = r == 2 * c + j

                    @pl.when(mine)
                    def _():
                        oin[l, s, at_multiple(r, hb), :] = ob[l, s, :, pl.ds(j * ks, ks)]

                    @pl.when(jnp.logical_not(mine))
                    def _():
                        copy.start()
                else:
                    copy.start()

    def on_own_column(full, short, wait, sem):
        @pl.when(chip == c)
        def _():
            wait(short, sem)

        @pl.when(chip != c)
        def _():
            wait(full, sem)

    def add_block(x, update):
        block = x[:, at_multiple(c, cw)].astype(F32)
        return (block + update.astype(BF16).astype(F32)).astype(BF16)

    def gather_cols(dst, block, send_sem, recv_sem):
        dst[:, at_multiple(c, cw)] = block
        for d in range(1, cols_n):
            peer_copy(dst.at[:, at_multiple(c, cw)], dst.at[:, at_multiple(c, cw)], send_sem, recv_sem,
                      r, lax.rem(c + d, cols_n)).start()

    def layer(l, carry):
        for s in range(STEPS):
            if s == 0:
                for src, lo, n in ((wq, 0, q_w), (wk, q_w, kv_w), (wv, q_w + kv_w, kv_w)):
                    pltpu.make_async_copy(src.at[l], wqkv.at[l, :, pl.ds(lo, n)], w_sem.at[l, 0]).wait()
            wait_recv(nin1.at[l, s, pl.ds(0, batch - hb), :], n1_recv.at[l, s])
            qs[l, s] = jnp.dot(nin1[l, s], wqkv[l], preferred_element_type=F32).astype(BF16)
            scatter_rows(qs, qr, q_send, q_recv, l, s)
        for s in range(STEPS):
            if s == 0:
                pltpu.make_async_copy(kc.at[l], kbuf.at[l], kv_sem.at[l, 0]).wait()
                pltpu.make_async_copy(vc.at[l], vbuf.at[l], kv_sem.at[l, 1]).wait()
            attention(l, s)
        for s in range(STEPS):
            if s == 0:
                pltpu.make_async_copy(wo.at[l], wov.at[l], w_sem.at[l, 1]).wait()
            on_own_column(oin.at[l, s], oin.at[l, s, pl.ds(0, batch - hb), :], wait_recv, o_recv.at[l, s])
            os_[l, s] = jnp.dot(oin[l, s], wov[l], preferred_element_type=F32).astype(BF16)
            scatter_rows(os_, orr, ro_send, ro_recv, l, s)
        for s in range(STEPS):
            total = reduce_rows(os_, orr, ro_recv, l, s)
            gather_cols(xmid.at[l, s], add_block(xst.at[l, s], total), x_send.at[l, s], x_recv.at[l, s])
        for s in range(STEPS):
            wait_recv(xmid.at[l, s, :, pl.ds(0, width - cw)], x_recv.at[l, s])
            nst2[l, s] = norm_rows(xmid[l, s], layers + l)
            for d in range(1, rows_n):
                to = row_peer(d)
                peer_copy(nst2.at[l, s, :, at_multiple(to // 2, 2 * ks)], nin2.at[l, s, at_multiple(r, hb), :],
                          n2_send.at[l, s], n2_recv.at[l, s], to, c).start()
            nin2[l, s, at_multiple(r, hb), :] = nst2[l, s, :, at_multiple(chip, 2 * ks)]
        for s in range(STEPS):
            if s == 0:
                for k, src in enumerate((wg, wu)):
                    pltpu.make_async_copy(src.at[l, :, at_multiple(core, fh)],
                                          wgu.at[l, at_multiple(core, ks), pl.ds(k * fh, fh)], w_sem.at[l, 2]).wait()
                wait_recv(wgu.at[l, pl.ds(0, ks), :], wx_recv.at[l])
            wait_recv(nin2.at[l, s, pl.ds(0, batch - hb), :], n2_recv.at[l, s])
            tile = 512

            def columns(k, carry):
                gs[l, s, :, at_multiple(k, tile)] = jnp.dot(
                    nin2[l, s], wgu[l, :, at_multiple(k, tile)], preferred_element_type=F32).astype(BF16)
                return carry

            lax.fori_loop(0, 2 * fh // tile, columns, 0)
            for d in range(1, chips_n):
                to = lax.rem(chip + d, chips_n)
                peer_copy(gs.at[l, s, at_multiple(to, cb), :], gr.at[l, s, d - 1],
                          gu_send.at[l, s], gu_recv.at[l, s], 2 * to + core, c).start()
        for s in range(STEPS):
            wait_recv(gr.at[l, s], gu_recv.at[l, s])
            total = gs[l, s, at_multiple(chip, cb), :].astype(F32)
            for d in range(chips_n - 1):
                total += gr[l, s, d].astype(F32)
            total = total.astype(BF16).astype(F32)
            gate, up = total[:, :fh], total[:, fh:]
            aa[l, s, c] = (gate / (1.0 + jnp.exp(-gate)) * up).astype(BF16)
            for d in range(1, cols_n):
                peer_copy(aa.at[l, s, c], aa.at[l, s, c], aa_send.at[l, s], aa_recv.at[l, s, c],
                          r, lax.rem(c + d, cols_n)).start()
        for s in range(STEPS):
            for d in (1, 2, 3, 0):
                to = lax.rem(chip + d, chips_n)

                @pl.when(to != c)
                def _():
                    wait_recv(aa.at[l, s, to], aa_recv.at[l, s, to])

                if d:
                    peer_copy(aa.at[l, s, to], ab.at[l, s, at_multiple(chip, cb), :],
                              ab_send.at[l, s], ab_recv.at[l, s], 2 * to + core, c).start()
                else:
                    ab[l, s, at_multiple(chip, cb), :] = aa[l, s, to]
        for s in range(STEPS):
            if s == 0:
                pltpu.make_async_copy(wd.at[l], wdv.at[l], w_sem.at[l, 3]).wait()
            wait_recv(ab.at[l, s, pl.ds(0, batch - cb), :], ab_recv.at[l, s])
            ds_[l, s] = jnp.dot(ab[l, s], wdv[l], preferred_element_type=F32).astype(BF16)
            scatter_rows(ds_, dr, rd_send, rd_recv, l, s)
        for s in range(STEPS):
            total = reduce_rows(ds_, dr, rd_recv, l, s)
            gather_cols(xst.at[l + 1, s], add_block(xmid.at[l, s], total), x2_send.at[l, s], x2_recv.at[l, s])
        last = l == layers - 1
        for s in range(STEPS):
            wait_recv(xst.at[l + 1, s, :, pl.ds(0, width - cw)], x2_recv.at[l, s])
            x = xst[l + 1, s]
            nst1[l + 1, s] = jnp.where(last, x, norm_rows(x, jnp.minimum(l + 1, layers - 1)))
            send_n1(l + 1, s)
        return carry

    lax.fori_loop(0, layers, layer, 0)

    for s in range(STEPS):
        wait_recv(nin1.at[layers, s, pl.ds(0, batch - hb), :], n1_recv.at[layers, s])
        pltpu.make_async_copy(nin1.at[layers, s], outs[s], out_sem.at[s]).start()

    for d in range(1, rows_n):
        wait_send(gsrc, g_send)
    for s in range(STEPS):
        wait_send(hin.at[s, pl.ds(0, batch - hb), :], init_send.at[s])

    def finish(l, carry):
        wait_send(wgu.at[l, pl.ds(0, ks), :], wx_send.at[l])
        for s in range(STEPS):
            wait_send(nin1.at[l, s, pl.ds(0, batch - hb), :], n1_send.at[l, s])
            wait_send(qr.at[l, s], q_send.at[l, s])
            on_own_column(oin.at[l, s], oin.at[l, s, pl.ds(0, batch - hb), :], wait_send, o_send.at[l, s])
            wait_send(orr.at[l, s], ro_send.at[l, s])
            wait_send(xmid.at[l, s, :, pl.ds(0, width - cw)], x_send.at[l, s])
            wait_send(nin2.at[l, s, pl.ds(0, batch - hb), :], n2_send.at[l, s])
            wait_send(gr.at[l, s], gu_send.at[l, s])
            wait_send(aa.at[l, s, pl.ds(0, cols_n - 1)], aa_send.at[l, s])
            wait_send(ab.at[l, s, pl.ds(0, batch - cb), :], ab_send.at[l, s])
            wait_send(dr.at[l, s], rd_send.at[l, s])
            wait_send(xst.at[l + 1, s, :, pl.ds(0, width - cw)], x2_send.at[l, s])
        return carry

    lax.fori_loop(0, layers, finish, 0)
    for s in range(STEPS):
        wait_send(nin1.at[layers, s, pl.ds(0, batch - hb), :], n1_send.at[layers, s])
        pltpu.make_async_copy(nin1.at[layers, s], outs[s], out_sem.at[s]).wait()


def cache_kernel(lens, new_kv, kc, vc, ko, vo, buf, in_sem, out_sem):
    layers, seqs = kc.shape[0], kc.shape[1]
    caches, results = (kc, vc), (ko, vo)

    def load(i, carry):
        l, b = i // seqs, lax.rem(i, seqs)
        for w in range(2):
            pltpu.make_async_copy(caches[w].at[l, b], buf.at[w, i], in_sem.at[w, i]).start()
        return carry

    def store(i, carry):
        l, b = i // seqs, lax.rem(i, seqs)
        first = lens[b]
        rows = lax.broadcasted_iota(jnp.int32, (8, 128), 0)
        lane = lax.broadcasted_iota(jnp.int32, (kc.shape[2], 128), 1)
        for w in range(2):
            pltpu.make_async_copy(caches[w].at[l, b], buf.at[w, i], in_sem.at[w, i]).wait()
            for s in range(STEPS):
                row = jnp.broadcast_to(new_kv[l, s, w, pl.ds(b, 1), :], (8, 128))
                spread = lax.dot_general(jnp.where(rows == 0, row, 0.0).astype(BF16), jnp.ones((8, 128), BF16),
                                         (((0,), (0,)), ((), ())), preferred_element_type=F32)
                slot = first + s
                window = pl.ds(pl.multiple_of(slot // 128 * 128, 128), 128)
                old = buf[w, i, :, window].astype(F32)
                buf[w, i, :, window] = jnp.where(lane == lax.rem(slot, 128), spread, old).astype(BF16)
            pltpu.make_async_copy(buf.at[w, i], results[w].at[l, b], out_sem).start()
        return carry

    lax.fori_loop(0, layers * seqs, load, 0)
    lax.fori_loop(0, layers * seqs, store, 0)

    def drain(i, carry):
        l, b = i // seqs, lax.rem(i, seqs)
        for w in range(2):
            pltpu.make_async_copy(buf.at[w, i], results[w].at[l, b], out_sem).wait()
        return carry

    lax.fori_loop(0, layers * seqs, drain, 0)


def solution(mesh):
    rows_n, cols_n = mesh.shape['row'], mesh.shape['col']
    chips_n = rows_n // 2
    hidden_spec = P('rep', 'row')
    index_spec = P(('rep', 'row'))
    cache_spec = P(None, ('rep', 'row'), None, 'col', None)
    gain_spec = P(None, 'row')
    weight_spec = P(None, 'row', 'col')

    def device_program(h0, h1, pos, lens, cache_k, cache_v, gain_a, gain_m, wq, wk, wv, wo, wg, wu, wd):
        layers, seqs, ctx, heads, dim = cache_k.shape
        batch, ks = h0.shape
        hb, cb = batch // rows_n, batch // chips_n
        width = ks * rows_n
        cw, q_w, kv_w, ff = wo.shape[-1], wq.shape[-1], wk.shape[-1], wg.shape[-1]
        qkv_w = q_w + 2 * kv_w
        kc, vc = (jnp.transpose(x, (0, 1, 3, 4, 2)).reshape(layers, seqs, heads * dim, ctx) for x in (cache_k, cache_v))
        half = dim // 2
        table = ROPE_BASE ** (-(np.arange(128) % half) * 2.0 / dim)
        freq = jnp.asarray(table.reshape(1, 128), F32)
        vmem = pl.BlockSpec(memory_space=pltpu.VMEM)
        smem = pl.BlockSpec(memory_space=pltpu.SMEM)
        hbm = pl.BlockSpec(memory_space=pl.ANY)
        dma = pltpu.SemaphoreType.DMA

        def buf(*shape, dtype=BF16):
            return pltpu.VMEM(shape, dtype)

        ls = (layers, STEPS)
        ls1 = (layers + 1, STEPS)
        scratch = [
            buf(STEPS, batch, ks), buf(8, ks, dtype=F32), buf(8, width, dtype=F32),
            buf(layers, seqs, kv_w, ctx), buf(layers, seqs, kv_w, ctx),
            buf(layers, ks, qkv_w), buf(layers, ks, cw), buf(layers, 2 * ks, ff), buf(layers, *wd.shape[1:]),
            buf(*ls1, hb, width), buf(*ls, hb, width), buf(*ls1, hb, width), buf(*ls1, batch, ks),
            buf(*ls, batch, qkv_w), buf(*ls, rows_n - 1, hb, qkv_w),
            buf(*ls, hb, q_w), buf(*ls, batch, ks),
            buf(*ls, batch, cw), buf(*ls, rows_n - 1, hb, cw),
            buf(*ls, hb, width), buf(*ls, batch, 2 * ks),
            buf(*ls, batch, ff), buf(*ls, chips_n - 1, cb, ff),
            buf(*ls, cols_n, cb, ff // 2), buf(*ls, batch, ff // 2),
            buf(*ls, batch, cw), buf(*ls, rows_n - 1, hb, cw),
            buf(hb * 8, 128, dtype=F32), buf(hb * 8, 128, dtype=F32),
            buf(STEPS, hb, kv_w, dtype=F32), buf(STEPS, hb, kv_w, dtype=F32),
            buf(STEPS, hb, 128, dtype=F32), buf(STEPS, hb, 128, dtype=F32),
            dma((STEPS,)), dma((layers, 2)), dma((layers, 4)), dma((layers,)), dma((layers,)),
            dma((STEPS,)), dma((STEPS,)), dma(()), dma(()),
            dma(ls1), dma(ls1), dma(ls), dma(ls), dma(ls), dma(ls), dma(ls), dma(ls), dma(ls), dma(ls),
            dma(ls), dma(ls), dma(ls), dma(ls), dma(ls), dma((*ls, cols_n)), dma(ls), dma(ls), dma(ls), dma(ls),
            dma(ls), dma(ls), dma((STEPS,)),
        ]
        out_0, out_1, new_kv = pl.pallas_call(
            decode_kernel,
            out_shape=(jax.ShapeDtypeStruct(h0.shape, BF16), jax.ShapeDtypeStruct(h1.shape, BF16),
                       jax.ShapeDtypeStruct((layers, STEPS, 2, seqs, kv_w), F32)),
            in_specs=[hbm, hbm, smem, smem, hbm, hbm, vmem, vmem, vmem] + [hbm] * 7,
            out_specs=(hbm, hbm, vmem),
            scratch_shapes=scratch,
            compiler_params=pltpu.CompilerParams(collective_id=0, has_side_effects=True,
                                                 vmem_limit_bytes=58 * 1024 * 1024),
            name='decode',
        )(h0, h1, pos, lens, kc, vc, gain_a, gain_m, freq, wq, wk, wv, wo, wg, wu, wd)
        ko, vo = pl.pallas_call(
            cache_kernel,
            out_shape=(jax.ShapeDtypeStruct(kc.shape, BF16),) * 2,
            in_specs=[smem, vmem, hbm, hbm],
            out_specs=(hbm, hbm),
            scratch_shapes=[buf(2, layers * seqs, kv_w, ctx), dma((2, layers * seqs)), dma(())],
            compiler_params=pltpu.CompilerParams(vmem_limit_bytes=40 * 1024 * 1024),
            name='cache',
        )(lens, new_kv, kc, vc)
        ko, vo = (jnp.transpose(x.reshape(layers, seqs, heads, dim, ctx), (0, 1, 4, 2, 3)) for x in (ko, vo))
        return out_0, out_1, ko, vo

    return jax.shard_map(device_program, mesh=mesh,
                         in_specs=(hidden_spec, hidden_spec, index_spec, index_spec, cache_spec, cache_spec,
                                   gain_spec, gain_spec) + (weight_spec,) * 7,
                         out_specs=(hidden_spec, hidden_spec, cache_spec, cache_spec), check_vma=False)
```

```python
import functools

import jax
import jax.numpy as jnp
import numpy as np
from jax import lax
from jax.experimental import pallas as pl
from jax.experimental.pallas import tpu as pltpu
from jax.sharding import PartitionSpec as P

ROPE_BASE = 1000000.0
EPS = 1e-05
MESH = pl.DeviceIdType.MESH
BF16 = jnp.bfloat16
F32 = jnp.float32
STEPS = 2
CHUNKS = 4


def at_multiple(index, size):
    return pl.ds(pl.multiple_of(index * size, size), size)


def decode_kernel(
        h0, h1, pos_in, lens_in, kc, vc, gain_a_in, gain_m_in, freq_in, wq, wk, wv, wo, wg, wu, wd,
        out0, out1, kbuf, vbuf,
        hin, pos, lens, gain_a, gain_m, freq, gsrc, gful, sq, sqr, wqkv, wov, wgu, wdv,
        xst, xmid, nst1, nin1, qs, qr, ob, oin, os_, orr, nst2, nin2, gs, gr, aa, ab, ds_, dr,
        qf, of, kn, vn, cs, sn,
        hin_sem, small_sem, sq_send, sq_recv, kv_sem, w_sem, wx_send, wx_recv, init_send, init_recv, g_send, g_recv,
        n1_send, n1_recv, q_send, q_recv, o_send, o_recv, ro_send, ro_recv, x_send, x_recv,
        n2_send, n2_recv, gu_send, gu_recv, aa_send, aa_recv, ab_send, ab_recv, rd_send, rd_recv,
        x2_send, x2_recv):
    layers = wq.shape[0]
    rows_n = lax.axis_size('row')
    cols_n = lax.axis_size('col')
    chips_n = rows_n // 2
    r = lax.axis_index('row')
    c = lax.axis_index('col')
    chip, core = r // 2, r % 2
    batch, ks = h0.shape
    hb = batch // rows_n
    width = ks * rows_n
    cw = wo.shape[-1]
    q_w = wq.shape[-1]
    kv_w = wk.shape[-1]
    qkv_w = q_w + 2 * kv_w
    ff = wg.shape[-1]
    fh = ff // 2
    cb = batch // chips_n
    fc = fh // CHUNKS
    ctx = kc.shape[-1]
    hins = (h0, h1)
    outs = (out0, out1)

    def peer_copy(src, dst, send_sem, recv_sem, row, col):
        return pltpu.make_async_remote_copy(
            src_ref=src, dst_ref=dst, send_sem=send_sem, recv_sem=recv_sem,
            device_id={'row': row, 'col': col}, device_id_type=MESH)

    def wait_recv(ref, sem):
        peer_copy(ref, ref, sem, sem, r, c).wait_recv()

    def wait_send(ref, sem):
        peer_copy(ref, ref, sem, sem, r, c).wait_send()

    def gate_up(l, k, half):
        columns = pl.ds(pl.multiple_of(half * fh + k // 2 * fc, fc), fc)
        return (wg, wu)[k % 2].at[l, :, columns], wgu.at[l, at_multiple(core, ks), pl.ds(k * fc, fc)]

    small = [pltpu.make_async_copy(src, dst, small_sem.at[k]) for k, (src, dst) in enumerate(
        ((gain_a_in, gain_a), (gain_m_in, gain_m), (freq_in, freq), (pos_in, pos), (lens_in, lens)))]
    for s in range(STEPS):
        pltpu.make_async_copy(hins[s], hin.at[s], hin_sem.at[s]).start()
    for copy in small:
        copy.start()
    for l in range(layers):
        for src, lo, n in ((wq, 0, q_w), (wk, q_w, kv_w), (wv, q_w + kv_w, kv_w)):
            pltpu.make_async_copy(src.at[l], wqkv.at[l, :, pl.ds(lo, n)], w_sem.at[l, 0]).start()
        pltpu.make_async_copy(kc.at[l], kbuf.at[l], kv_sem.at[l, 0]).start()
        pltpu.make_async_copy(vc.at[l], vbuf.at[l], kv_sem.at[l, 1]).start()
        pltpu.make_async_copy(wo.at[l], wov.at[l], w_sem.at[l, 1]).start()
        for k in range(2 * CHUNKS):
            pltpu.make_async_copy(*gate_up(l, k, core), w_sem.at[l, 2]).start()
        pltpu.make_async_copy(wd.at[l], wdv.at[l], w_sem.at[l, 3]).start()

    barrier = pltpu.get_barrier_semaphore()
    for k in range(1, rows_n * cols_n):
        other = lax.rem(r * cols_n + c + k, rows_n * cols_n)
        pl.semaphore_signal(barrier, inc=1, device_id={'row': other // cols_n, 'col': lax.rem(other, cols_n)},
                            device_id_type=MESH)
    pl.semaphore_wait(barrier, rows_n * cols_n - 1)

    def row_peer(d):
        return lax.rem(r + d, rows_n)

    def row_sums(s):
        xf = hin[s].astype(F32)
        return jnp.sum(xf * xf, axis=-1, keepdims=True)

    for s in range(STEPS):
        pltpu.make_async_copy(hins[s], hin.at[s], hin_sem.at[s]).wait()
        sq[s] = jnp.transpose(jnp.broadcast_to(row_sums(s), (batch, batch)))[:8]
        for d in range(1, rows_n):
            peer_copy(sq.at[s], sqr.at[s, d - 1], sq_send.at[s], sq_recv.at[s], row_peer(d), c).start()
    for s in range(STEPS):
        for d in range(1, rows_n):
            peer_copy(hin.at[s, at_multiple(row_peer(d), hb), :], xst.at[0, s, :, at_multiple(r, ks)],
                      init_send.at[s], init_recv.at[s], row_peer(d), c).start()
        xst[0, s, :, at_multiple(r, ks)] = hin[s, at_multiple(r, hb), :]
    for copy in small:
        copy.wait()
    gsrc[...] = jnp.concatenate([gain_a[...].astype(F32), gain_m[...].astype(F32),
                                 jnp.zeros((gsrc.shape[0] - 2 * layers, ks), F32)], axis=0)
    gful[:, at_multiple(r, ks)] = gsrc[...]
    for d in range(1, rows_n):
        peer_copy(gsrc, gful.at[:, at_multiple(r, ks)], g_send, g_recv, row_peer(d), c).start()
    for l in range(layers):
        for k in range(2 * CHUNKS):
            peer_copy(*gate_up(l, k, 1 - core), wx_send.at[l], wx_recv.at[l], r + 1 - 2 * core, c).start()

    lane = lax.broadcasted_iota(jnp.int32, (hb, 128), 1)
    sub = lax.broadcasted_iota(jnp.int32, (hb, 128), 0)
    first_half = lax.rem(lane, 64) < 32
    pos_col = jnp.zeros((hb, 128), jnp.int32)
    for b in range(hb):
        pos_col = jnp.where(sub == b, pos[b], pos_col)
    for s in range(STEPS):
        angle = (pos_col + s).astype(F32) * freq[...]
        cs[s] = jnp.cos(angle)
        sine = jnp.sin(angle)
        sn[s] = jnp.where(first_half, -sine, sine)

    def norm_rows(x, gain_row):
        xf = x.astype(F32)
        scale = lax.rsqrt(jnp.sum(xf * xf, axis=-1, keepdims=True) * (1.0 / width) + EPS)
        return (xf * scale * gful[pl.ds(gain_row, 1), :]).astype(BF16)

    def send_n1(l, s):
        for d in range(1, rows_n):
            peer_copy(nst1.at[l, s, :, at_multiple(row_peer(d), ks)], nin1.at[l, s, at_multiple(r, hb), :],
                      n1_send.at[l, s], n1_recv.at[l, s], row_peer(d), c).start()
        nin1[l, s, at_multiple(r, hb), :] = nst1[l, s, :, at_multiple(r, ks)]

    for s in range(STEPS):
        wait_recv(sqr.at[s], sq_recv.at[s])
        total = sq[s]
        for d in range(rows_n - 1):
            total += sqr[s, d]
        total = jnp.transpose(jnp.broadcast_to(total[:1], (batch, batch)))[:, :1]
        scale = lax.rsqrt(total * (1.0 / width) + EPS)
        nin1[0, s] = (hin[s].astype(F32) * scale * gain_a[:1, :].astype(F32)).astype(BF16)

    def reduce_rows(stage, recv, sem, l, s):
        wait_recv(recv.at[l, s], sem.at[l, s])
        total = stage[l, s, at_multiple(r, hb), :].astype(F32)
        for d in range(rows_n - 1):
            total += recv[l, s, d].astype(F32)
        return total

    def scatter_rows(stage, recv, send_sem, recv_sem, l, s):
        for d in range(1, rows_n):
            peer_copy(stage.at[l, s, at_multiple(row_peer(d), hb), :], recv.at[l, s, d - 1],
                      send_sem.at[l, s], recv_sem.at[l, s], row_peer(d), c).start()

    def rope(x, s):
        turned = jnp.where(first_half, pltpu.roll(x, 96, 1), pltpu.roll(x, 32, 1))
        return (x * cs[s] + turned * sn[s]).astype(BF16).astype(F32)

    def attention(l, s):
        qkv = reduce_rows(qs, qr, q_recv, l, s).astype(BF16).astype(F32)
        key = rope(qkv[:, q_w:q_w + kv_w], s)
        val = qkv[:, q_w + kv_w:]
        kn[s] = key
        vn[s] = val
        for t in range(4):
            kv, pair = t // 2, t % 2
            y = rope(qkv[:, 128 * t:128 * t + 128], s)
            for e in range(2):
                z = y if e == kv else pltpu.roll(y, 64, 1)
                qf[pl.ds(kv * 4 + pair * 2 + e, hb, stride=8), :] = jnp.where(lane // 64 == kv, z, 0.0)
        slot = lax.broadcasted_iota(jnp.int32, (8, ctx), 1)

        def group(gi, carry):
            for u in range(4):
                b = gi * 4 + u
                qv = qf[at_multiple(b, 8), :]
                sc = jnp.dot(qv.astype(BF16), kbuf[l, b], preferred_element_type=F32) * 0.125
                sc = jnp.where(slot < lens[b], sc, -jnp.inf)
                top = jnp.max(sc, axis=-1, keepdims=True)
                news = []
                for e in range(s + 1):
                    news.append(jnp.sum(qv * kn[e, pl.ds(b, 1), :], axis=-1, keepdims=True) * 0.125)
                    top = jnp.maximum(top, news[e])
                p = jnp.exp(sc - top)
                news = [jnp.exp(x - top) for x in news]
                inv = 1.0 / functools.reduce(lambda x, y: x + y, news, jnp.sum(p, axis=-1, keepdims=True))
                o = lax.dot_general((p * inv).astype(BF16), vbuf[l, b], (((1,), (1,)), ((), ())),
                                    preferred_element_type=F32)
                for e in range(s + 1):
                    o += (news[e] * inv).astype(BF16).astype(F32) * vn[e, pl.ds(b, 1), :]
                of[at_multiple(b, 8), :] = o
            return carry

        lax.fori_loop(0, hb // 4, group, 0)
        for t in range(4):
            kv, pair = t // 2, t % 2
            lo = of[pl.ds(kv * 4 + pair * 2, hb, stride=8), :]
            hi = of[pl.ds(kv * 4 + pair * 2 + 1, hb, stride=8), :]
            lo = lo if kv == 0 else pltpu.roll(lo, 64, 1)
            hi = hi if kv == 1 else pltpu.roll(hi, 64, 1)
            ob[l, s, :, 128 * t:128 * t + 128] = jnp.where(lane < 64, lo, hi).astype(BF16)
        for j in range(2):
            for d in range(cols_n):
                copy = peer_copy(ob.at[l, s, :, pl.ds(j * ks, ks)], oin.at[l, s, at_multiple(r, hb), :],
                                 o_send.at[l, s], o_recv.at[l, s], 2 * c + j, lax.rem(c + d, cols_n))
                if d == 0:
                    mine = r == 2 * c + j

                    @pl.when(mine)
                    def _():
                        oin[l, s, at_multiple(r, hb), :] = ob[l, s, :, pl.ds(j * ks, ks)]

                    @pl.when(jnp.logical_not(mine))
                    def _():
                        copy.start()
                else:
                    copy.start()

    def insert_new(l):
        sub8 = lax.broadcasted_iota(jnp.int32, (8, kv_w), 0)
        slot = lax.broadcasted_iota(jnp.int32, (8, ctx), 1)
        step = lax.broadcasted_iota(jnp.int32, (8, ctx), 0)
        wide = lax.broadcasted_iota(jnp.int32, (kv_w, ctx), 1)

        def one(b, carry):
            first = lens[b]
            at = jnp.where((step < STEPS) & (slot == first + step), 1.0, 0.0).astype(BF16)
            fresh = (wide >= first) & (wide < first + STEPS)
            for new, cache in ((kn, kbuf), (vn, vbuf)):
                rows = jnp.where(sub8 == 0, new[0, pl.ds(b, 1), :], jnp.where(sub8 == 1, new[1, pl.ds(b, 1), :], 0.0))
                spread = lax.dot_general(rows.astype(BF16), at, (((0,), (0,)), ((), ())), preferred_element_type=F32)
                cache[l, b] = jnp.where(fresh, spread, cache[l, b].astype(F32)).astype(BF16)
            return carry

        lax.fori_loop(0, hb, one, 0)

    def on_own_column(full, short, wait, sem):
        @pl.when(chip == c)
        def _():
            wait(short, sem)

        @pl.when(chip != c)
        def _():
            wait(full, sem)

    def add_block(x, update):
        block = x[:, at_multiple(c, cw)].astype(F32)
        return (block + update.astype(BF16).astype(F32)).astype(BF16)

    def gather_cols(dst, block, send_sem, recv_sem):
        dst[:, at_multiple(c, cw)] = block
        for d in range(1, cols_n):
            peer_copy(dst.at[:, at_multiple(c, cw)], dst.at[:, at_multiple(c, cw)], send_sem, recv_sem,
                      r, lax.rem(c + d, cols_n)).start()

    def layer(l, carry):
        for s in range(STEPS):
            if s == 0:
                for src, lo, n in ((wq, 0, q_w), (wk, q_w, kv_w), (wv, q_w + kv_w, kv_w)):
                    pltpu.make_async_copy(src.at[l], wqkv.at[l, :, pl.ds(lo, n)], w_sem.at[l, 0]).wait()
            @pl.when(l > 0)
            def _():
                wait_recv(nin1.at[l, s, pl.ds(0, batch - hb), :], n1_recv.at[l, s])

            qs[l, s] = jnp.dot(nin1[l, s], wqkv[l], preferred_element_type=F32).astype(BF16)
            scatter_rows(qs, qr, q_send, q_recv, l, s)
        for s in range(STEPS):
            if s == 0:
                pltpu.make_async_copy(kc.at[l], kbuf.at[l], kv_sem.at[l, 0]).wait()
                pltpu.make_async_copy(vc.at[l], vbuf.at[l], kv_sem.at[l, 1]).wait()
            attention(l, s)
        for s in range(STEPS):
            if s == 0:
                pltpu.make_async_copy(wo.at[l], wov.at[l], w_sem.at[l, 1]).wait()
            on_own_column(oin.at[l, s], oin.at[l, s, pl.ds(0, batch - hb), :], wait_recv, o_recv.at[l, s])
            os_[l, s] = jnp.dot(oin[l, s], wov[l], preferred_element_type=F32).astype(BF16)
            scatter_rows(os_, orr, ro_send, ro_recv, l, s)
        for s in range(STEPS):
            @pl.when(l == 0)
            def _():
                wait_recv(xst.at[0, s, :, pl.ds(0, (rows_n - 1) * ks)], init_recv.at[s])

            total = reduce_rows(os_, orr, ro_recv, l, s)
            gather_cols(xmid.at[l, s], add_block(xst.at[l, s], total), x_send.at[l, s], x_recv.at[l, s])
        for s in range(STEPS):
            if s == 0:
                @pl.when(l == 0)
                def _():
                    wait_recv(gful.at[:, pl.ds(0, (rows_n - 1) * ks)], g_recv)

            wait_recv(xmid.at[l, s, :, pl.ds(0, width - cw)], x_recv.at[l, s])
            nst2[l, s] = norm_rows(xmid[l, s], layers + l)
            for d in range(1, rows_n):
                to = row_peer(d)
                peer_copy(nst2.at[l, s, :, at_multiple(to // 2, 2 * ks)], nin2.at[l, s, at_multiple(r, hb), :],
                          n2_send.at[l, s], n2_recv.at[l, s], to, c).start()
            nin2[l, s, at_multiple(r, hb), :] = nst2[l, s, :, at_multiple(chip, 2 * ks)]
        for s in range(STEPS):
            if s == 0:
                for k in range(2 * CHUNKS):
                    pltpu.make_async_copy(*gate_up(l, k, core), w_sem.at[l, 2]).wait()
                wait_recv(wgu.at[l, pl.ds(0, ks), :], wx_recv.at[l])
            wait_recv(nin2.at[l, s, pl.ds(0, batch - hb), :], n2_recv.at[l, s])
            for k in range(CHUNKS):
                columns = pl.ds(k * 2 * fc, 2 * fc)
                gs[l, s, :, columns] = jnp.dot(nin2[l, s], wgu[l, :, columns], preferred_element_type=F32).astype(BF16)
                for d in range(1, chips_n):
                    to = lax.rem(chip + d, chips_n)
                    peer_copy(gs.at[l, s, at_multiple(to, cb), columns], gr.at[l, s, d - 1, :, columns],
                              gu_send.at[l, s], gu_recv.at[l, s, k], 2 * to + core, c).start()
        insert_new(l)

        def activate(s, k):
            columns = pl.ds(k * 2 * fc, 2 * fc)
            wait_recv(gr.at[l, s, :, :, columns], gu_recv.at[l, s, k])
            total = gs[l, s, at_multiple(chip, cb), columns].astype(F32)
            for d in range(chips_n - 1):
                total += gr[l, s, d, :, columns].astype(F32)
            total = total.astype(BF16).astype(F32)
            gate, up = total[:, :fc], total[:, fc:]
            part = pl.ds(k * fc, fc)
            aa[l, s, c, :, part] = (gate / (1.0 + jnp.exp(-gate)) * up).astype(BF16)
            for d in range(1, cols_n):
                peer_copy(aa.at[l, s, c, :, part], aa.at[l, s, c, :, part], aa_send.at[l, s], aa_recv.at[l, s, k, c],
                          r, lax.rem(c + d, cols_n)).start()

        def relay(s, k):
            part = pl.ds(k * fc, fc)
            for d in (1, 2, 3, 0):
                to = lax.rem(chip + d, chips_n)

                @pl.when(to != c)
                def _():
                    wait_recv(aa.at[l, s, to, :, part], aa_recv.at[l, s, k, to])

                if d:
                    peer_copy(aa.at[l, s, to, :, part], ab.at[l, s, at_multiple(chip, cb), part],
                              ab_send.at[l, s], ab_recv.at[l, s], 2 * to + core, c).start()
                else:
                    ab[l, s, at_multiple(chip, cb), part] = aa[l, s, to, :, part]

        work = [(s, k) for s in range(STEPS) for k in range(CHUNKS)]
        lag = 2
        for t in range(len(work) + lag):
            if t < len(work):
                activate(*work[t])
            if t >= lag:
                relay(*work[t - lag])
        for s in range(STEPS):
            if s == 0:
                pltpu.make_async_copy(wd.at[l], wdv.at[l], w_sem.at[l, 3]).wait()
            wait_recv(ab.at[l, s, pl.ds(0, batch - cb), :], ab_recv.at[l, s])
            ds_[l, s] = jnp.dot(ab[l, s], wdv[l], preferred_element_type=F32).astype(BF16)
            scatter_rows(ds_, dr, rd_send, rd_recv, l, s)
        for s in range(STEPS):
            total = reduce_rows(ds_, dr, rd_recv, l, s)
            gather_cols(xst.at[l + 1, s], add_block(xmid.at[l, s], total), x2_send.at[l, s], x2_recv.at[l, s])
        last = l == layers - 1
        for s in range(STEPS):
            wait_recv(xst.at[l + 1, s, :, pl.ds(0, width - cw)], x2_recv.at[l, s])
            x = xst[l + 1, s]
            nst1[l + 1, s] = jnp.where(last, x, norm_rows(x, jnp.minimum(l + 1, layers - 1)))
            send_n1(l + 1, s)
        return carry

    lax.fori_loop(0, layers, layer, 0)

    for s in range(STEPS):
        wait_recv(nin1.at[layers, s, pl.ds(0, batch - hb), :], n1_recv.at[layers, s])
        outs[s][...] = nin1[layers, s]

    for d in range(1, rows_n):
        wait_send(gsrc, g_send)
    for s in range(STEPS):
        wait_send(sqr.at[s], sq_send.at[s])
        wait_send(hin.at[s, pl.ds(0, batch - hb), :], init_send.at[s])

    def finish(l, carry):
        wait_send(wgu.at[l, pl.ds(0, ks), :], wx_send.at[l])
        for s in range(STEPS):
            wait_send(nin1.at[l + 1, s, pl.ds(0, batch - hb), :], n1_send.at[l + 1, s])
            wait_send(qr.at[l, s], q_send.at[l, s])
            on_own_column(oin.at[l, s], oin.at[l, s, pl.ds(0, batch - hb), :], wait_send, o_send.at[l, s])
            wait_send(orr.at[l, s], ro_send.at[l, s])
            wait_send(xmid.at[l, s, :, pl.ds(0, width - cw)], x_send.at[l, s])
            wait_send(nin2.at[l, s, pl.ds(0, batch - hb), :], n2_send.at[l, s])
            wait_send(gr.at[l, s], gu_send.at[l, s])
            wait_send(aa.at[l, s, pl.ds(0, cols_n - 1)], aa_send.at[l, s])
            wait_send(ab.at[l, s, pl.ds(0, batch - cb), :], ab_send.at[l, s])
            wait_send(dr.at[l, s], rd_send.at[l, s])
            wait_send(xst.at[l + 1, s, :, pl.ds(0, width - cw)], x2_send.at[l, s])
        return carry

    lax.fori_loop(0, layers, finish, 0)


def solution(mesh):
    rows_n, cols_n = mesh.shape['row'], mesh.shape['col']
    chips_n = rows_n // 2
    hidden_spec = P('rep', 'row')
    index_spec = P(('rep', 'row'))
    cache_spec = P(None, ('rep', 'row'), None, 'col', None)
    gain_spec = P(None, 'row')
    weight_spec = P(None, 'row', 'col')

    def device_program(h0, h1, pos, lens, cache_k, cache_v, gain_a, gain_m, wq, wk, wv, wo, wg, wu, wd):
        layers, seqs, ctx, heads, dim = cache_k.shape
        batch, ks = h0.shape
        hb, cb = batch // rows_n, batch // chips_n
        width = ks * rows_n
        cw, q_w, kv_w, ff = wo.shape[-1], wq.shape[-1], wk.shape[-1], wg.shape[-1]
        qkv_w = q_w + 2 * kv_w
        kc, vc = (jnp.transpose(x, (0, 1, 3, 4, 2)).reshape(layers, seqs, heads * dim, ctx) for x in (cache_k, cache_v))
        half = dim // 2
        table = ROPE_BASE ** (-(np.arange(128) % half) * 2.0 / dim)
        freq = jnp.asarray(table.reshape(1, 128), F32)
        vmem = pl.BlockSpec(memory_space=pltpu.VMEM)
        hbm = pl.BlockSpec(memory_space=pltpu.HBM)
        dma = pltpu.SemaphoreType.DMA

        def buf(*shape, dtype=BF16):
            return pltpu.VMEM(shape, dtype)

        ls = (layers, STEPS)
        ls1 = (layers + 1, STEPS)
        scratch = [
            buf(STEPS, batch, ks), pltpu.SMEM(pos.shape, pos.dtype), pltpu.SMEM(lens.shape, lens.dtype),
            buf(*gain_a.shape), buf(*gain_m.shape), buf(1, 128, dtype=F32), buf(8, ks, dtype=F32), buf(8, width, dtype=F32),
            buf(STEPS, 8, batch, dtype=F32), buf(STEPS, rows_n - 1, 8, batch, dtype=F32),
            buf(layers, ks, qkv_w), buf(layers, ks, cw), buf(layers, 2 * ks, ff), buf(layers, *wd.shape[1:]),
            buf(*ls1, hb, width), buf(*ls, hb, width), buf(*ls1, hb, width), buf(*ls1, batch, ks),
            buf(*ls, batch, qkv_w), buf(*ls, rows_n - 1, hb, qkv_w),
            buf(*ls, hb, q_w), buf(*ls, batch, ks),
            buf(*ls, batch, cw), buf(*ls, rows_n - 1, hb, cw),
            buf(*ls, hb, width), buf(*ls, batch, 2 * ks),
            buf(*ls, batch, ff), buf(*ls, chips_n - 1, cb, ff),
            buf(*ls, cols_n, cb, ff // 2), buf(*ls, batch, ff // 2),
            buf(*ls, batch, cw), buf(*ls, rows_n - 1, hb, cw),
            buf(hb * 8, 128, dtype=F32), buf(hb * 8, 128, dtype=F32),
            buf(STEPS, hb, kv_w, dtype=F32), buf(STEPS, hb, kv_w, dtype=F32),
            buf(STEPS, hb, 128, dtype=F32), buf(STEPS, hb, 128, dtype=F32),
            dma((STEPS,)), dma((5,)), dma((STEPS,)), dma((STEPS,)), dma((layers, 2)), dma((layers, 4)), dma((layers,)), dma((layers,)),
            dma((STEPS,)), dma((STEPS,)), dma(()), dma(()),
            dma(ls1), dma(ls1), dma(ls), dma(ls), dma(ls), dma(ls), dma(ls), dma(ls), dma(ls), dma(ls),
            dma(ls), dma(ls), dma(ls), dma((*ls, CHUNKS)), dma(ls), dma((*ls, CHUNKS, cols_n)), dma(ls), dma(ls), dma(ls), dma(ls),
            dma(ls), dma(ls),
        ]
        out_0, out_1, ko, vo = pl.pallas_call(
            decode_kernel,
            out_shape=(pltpu.VMEM(h0.shape, BF16), pltpu.VMEM(h1.shape, BF16),
                       pltpu.VMEM(kc.shape, BF16), pltpu.VMEM(vc.shape, BF16)),
            in_specs=[hbm] * 16,
            out_specs=(vmem,) * 4,
            scratch_shapes=scratch,
            compiler_params=pltpu.CompilerParams(collective_id=0, has_side_effects=True,
                                                 vmem_limit_bytes=36 * 1024 * 1024),
            name='decode',
        )(*(pltpu.with_memory_space_constraint(x, pltpu.HBM)
            for x in (h0, h1, pos, lens, kc, vc, gain_a, gain_m, freq, wq, wk, wv, wo, wg, wu, wd)))
        ko, vo = (jnp.transpose(x.reshape(layers, seqs, heads, dim, ctx), (0, 1, 4, 2, 3)) for x in (ko, vo))
        return out_0, out_1, ko, vo

    return jax.shard_map(device_program, mesh=mesh,
                         in_specs=(hidden_spec, hidden_spec, index_spec, index_spec, cache_spec, cache_spec,
                                   gain_spec, gain_spec) + (weight_spec,) * 7,
                         out_specs=(hidden_spec, hidden_spec, cache_spec, cache_spec), check_vma=False)
```
